32 devices in a mesh: dp: 1 (over z), ep: 32 (over y, x, core).
Axes of the slice: x: 4, y: 4, z: 1, core: 2. Of those that a mesh axis runs over, the one named last changes fastest.
The devices are a block of a 4x4x8 slice.
Arguments:
- x_in: bfloat16 [96, 512, 2048], P(('dp', 'ep'))
- pad_mask: int32 [96, 512], P(('dp', 'ep'))
- rel_bias: float32 [16, 512, 512], replicated
- expert_idx: int32 [2, 96, 512], P(None, ('dp', 'ep'))
- norm_scale: float32 [2, 2, 2048], replicated
- w_query: bfloat16 [2, 2048, 2048], replicated
- w_key: bfloat16 [2, 2048, 2048], replicated
- w_value: bfloat16 [2, 2048, 2048], replicated
- w_attn_out: bfloat16 [2, 2048, 2048], replicated
- w_router: float32 [2, 2048, 64], replicated
- w_in: bfloat16 [2, 64, 2048, 1024], P(None, 'ep')
- w_out: bfloat16 [2, 64, 1024, 2048], P(None, 'ep')
Outputs:
- output: bfloat16 [96, 512, 2048], P(('dp', 'ep'))
All inputs are finite; a program needn't handle non-finite values.
Results may differ from the reference program's by a relative error of at most 0.019653.
Values are sent between devices in bfloat16 or wider.
A program may use at most 768 MiB of HBM per device.

```python
import jax
import jax.numpy as jnp
from jax import lax

SEQS = 3
SEQ = 512
D = 2048
HEADS = 16
HEAD = 128
FF = 1024
EXPERTS = 64
GROUPS = 32
CAP_FACTOR = 2
NORM_EPS = 1e-6
NEG_BIG = -1e9
TOKENS = SEQS * SEQ
NUM_SEQ = GROUPS * SEQS
INNER = HEADS * HEAD
CAPACITY = (CAP_FACTOR * TOKENS + EXPERTS - 1) // EXPERTS


def draw_mask(rng_key, num_seq):
    lengths = jax.random.randint(rng_key, (num_seq,), SEQ // 4, SEQ + 1)
    return (jnp.arange(SEQ)[None, :] < lengths[:, None]).astype(jnp.int32)


def draw_routes(rng_key, num_seq):
    route_keys = jax.random.split(rng_key, 5)
    rank_draws = [jax.random.randint(route_keys[draw_id], (2, num_seq, SEQ), 0, EXPERTS) for draw_id in range(3)]
    ranks = jnp.minimum(jnp.minimum(rank_draws[0], rank_draws[1]), rank_draws[2])
    perm_first = jax.random.permutation(route_keys[3], EXPERTS)
    perm_second = jax.random.permutation(route_keys[4], EXPERTS)
    return jnp.stack([perm_first[ranks[0]], perm_second[ranks[1]]]).astype(jnp.int32)


def setup_inputs(seed: int = 0, part: int = 0) -> dict:
    base_key = jax.random.key(seed)
    part_keys = jax.random.split(jax.random.fold_in(base_key, part), 3)
    shared_keys = jax.random.split(base_key, 10)
    x_in = jax.random.normal(part_keys[0], (NUM_SEQ, SEQ, D), jnp.float32).astype(jnp.bfloat16)
    pad_mask = draw_mask(part_keys[1], NUM_SEQ)
    expert_idx = draw_routes(part_keys[2], NUM_SEQ)
    rel_bias = 2.0 * jax.random.normal(shared_keys[0], (HEADS, SEQ, SEQ), jnp.float32)
    norm_scale = jax.random.uniform(shared_keys[1], (2, 2, D), jnp.float32, 0.5, 1.5)
    qk_std = (2.0 / D) ** 0.5 * HEAD ** -0.25
    w_query = (qk_std * jax.random.normal(shared_keys[2], (2, D, INNER), jnp.float32)).astype(jnp.bfloat16)
    w_key = (qk_std * jax.random.normal(shared_keys[3], (2, D, INNER), jnp.float32)).astype(jnp.bfloat16)
    w_value = (D ** -0.5 * jax.random.normal(shared_keys[4], (2, D, INNER), jnp.float32)).astype(jnp.bfloat16)
    w_attn_out = (INNER ** -0.5 * jax.random.normal(shared_keys[5], (2, INNER, D), jnp.float32)).astype(jnp.bfloat16)
    w_router = D ** -0.5 * jax.random.normal(shared_keys[6], (2, D, EXPERTS), jnp.float32)
    w_in = (D ** -0.5 * jax.random.normal(shared_keys[7], (2, EXPERTS, D, FF), jnp.float32)).astype(jnp.bfloat16)
    w_out = (EXPERTS * FF ** -0.5 * jax.random.normal(shared_keys[8], (2, EXPERTS, FF, D), jnp.float32)).astype(jnp.bfloat16)
    return dict(x_in=x_in, pad_mask=pad_mask, rel_bias=rel_bias, expert_idx=expert_idx, norm_scale=norm_scale, w_query=w_query, w_key=w_key, w_value=w_value, w_attn_out=w_attn_out, w_router=w_router, w_in=w_in, w_out=w_out)


def rms_norm(hidden, gain):
    hid32 = hidden.astype(jnp.float32)
    return hid32 * lax.rsqrt(jnp.mean(hid32 * hid32, axis=-1, keepdims=True) + NORM_EPS) * gain


def attention_block(hidden, pad_mask, rel_bias, gain, query_w, key_w, value_w, out_w):
    def one_sequence(seq_pair):
        seq_rows, seq_mask = seq_pair
        normed = rms_norm(seq_rows, gain).astype(jnp.bfloat16)
        query_rows = jnp.dot(normed, query_w, preferred_element_type=jnp.float32).astype(jnp.bfloat16).reshape(SEQ, HEADS, HEAD)
        key_rows = jnp.dot(normed, key_w, preferred_element_type=jnp.float32).astype(jnp.bfloat16).reshape(SEQ, HEADS, HEAD)
        value_rows = jnp.dot(normed, value_w, preferred_element_type=jnp.float32).astype(jnp.bfloat16).reshape(SEQ, HEADS, HEAD)
        scores = jnp.einsum('qhd,khd->hqk', query_rows.astype(jnp.float32), key_rows.astype(jnp.float32))
        scores = scores + rel_bias + jnp.where(seq_mask > 0, 0.0, NEG_BIG)[None, None, :]
        attn_probs = jax.nn.softmax(scores, axis=-1).astype(jnp.bfloat16)
        context = jnp.einsum('hqk,khd->qhd', attn_probs.astype(jnp.float32), value_rows.astype(jnp.float32))
        context = context.astype(jnp.bfloat16).reshape(SEQ, INNER)
        attn_out = jnp.dot(context, out_w, preferred_element_type=jnp.float32)
        return (seq_rows.astype(jnp.float32) + attn_out).astype(jnp.bfloat16)
    return lax.map(one_sequence, (hidden, pad_mask))


def expert_block(hidden, layer_ids, gain, route_w, up_w, down_w):
    grouped = hidden.reshape(GROUPS, TOKENS, D)
    ids_grouped = layer_ids.reshape(GROUPS, TOKENS)

    def route_group(grp_pair):
        grp_rows, grp_ids = grp_pair
        normed32 = rms_norm(grp_rows, gain)
        logits = jnp.dot(normed32, route_w, preferred_element_type=jnp.float32)
        gate_val = jnp.take_along_axis(jax.nn.softmax(logits, axis=-1), grp_ids[:, None], axis=1)[:, 0]
        one_hot = (grp_ids[:, None] == jnp.arange(EXPERTS)[None, :]).astype(jnp.int32)
        token_slot = jnp.take_along_axis(jnp.cumsum(one_hot, axis=0), grp_ids[:, None], axis=1)[:, 0] - 1
        flat_slot = jnp.where(token_slot < CAPACITY, grp_ids * CAPACITY + token_slot, EXPERTS * CAPACITY)
        slot_token = jnp.full((EXPERTS * CAPACITY,), TOKENS, jnp.int32).at[flat_slot].set(jnp.arange(TOKENS, dtype=jnp.int32), mode='drop')
        packed = jnp.take(normed32.astype(jnp.bfloat16), slot_token, axis=0, mode='fill', fill_value=0)
        return packed.reshape(EXPERTS, CAPACITY, D), gate_val, flat_slot

    packed, gate_val, flat_slot = lax.map(route_group, (grouped, ids_grouped))

    def one_expert(expert_parts):
        exp_rows, exp_up, exp_down = expert_parts
        flat_rows = exp_rows.reshape(GROUPS * CAPACITY, D)
        inner_act = jnp.maximum(jnp.dot(flat_rows, exp_up, preferred_element_type=jnp.float32), 0.0).astype(jnp.bfloat16)
        return jnp.dot(inner_act, exp_down, preferred_element_type=jnp.float32).astype(jnp.bfloat16).reshape(GROUPS, CAPACITY, D)

    expert_rows = lax.map(one_expert, (jnp.swapaxes(packed, 0, 1), up_w, down_w))
    expert_rows = jnp.swapaxes(expert_rows, 0, 1).reshape(GROUPS, EXPERTS * CAPACITY, D)

    def combine(grp_parts):
        grp_rows, grp_out, grp_gate, grp_flat = grp_parts
        returned = jnp.take(grp_out, grp_flat, axis=0, mode='fill', fill_value=0)
        return (grp_rows.astype(jnp.float32) + grp_gate[:, None] * returned.astype(jnp.float32)).astype(jnp.bfloat16)

    return lax.map(combine, (grouped, expert_rows, gate_val, flat_slot)).reshape(NUM_SEQ, SEQ, D)


def reference(x_in, pad_mask, rel_bias, expert_idx, norm_scale, w_query, w_key, w_value, w_attn_out, w_router, w_in, w_out):
    def layer_step(hidden, layer_params):
        gains, query_w, key_w, value_w, out_w, route_w, up_w, down_w, layer_ids = layer_params
        hidden = attention_block(hidden, pad_mask, rel_bias, gains[0], query_w, key_w, value_w, out_w)
        hidden = expert_block(hidden, layer_ids, gains[1], route_w, up_w, down_w)
        return hidden, None
    final_state = lax.scan(layer_step, x_in, (norm_scale, w_query, w_key, w_value, w_attn_out, w_router, w_in, w_out, expert_idx))
    return final_state[0]
```

```python
import functools

import jax
import jax.numpy as jnp
from jax import lax
from jax.experimental import pallas as pl
from jax.experimental.pallas import tpu as pltpu
from jax.sharding import PartitionSpec as P

NORM_EPS = 1e-6
NEG_BIG = -1e9
CAP_FACTOR = 2
HEADS_PER_STEP = 2


def rms_norm(hidden, gain):
    hid32 = hidden.astype(jnp.float32)
    return hid32 * lax.rsqrt(jnp.mean(hid32 * hid32, axis=-1, keepdims=True) + NORM_EPS) * gain


def attn_kernel(head_dim, q_ref, k_ref, v_ref, bias_ref, mask_ref, o_ref):
    mask = mask_ref[0]
    for head in range(bias_ref.shape[0]):
        cols = slice(head * head_dim, (head + 1) * head_dim)
        scores = lax.dot_general(q_ref[:, cols], k_ref[:, cols], (((1,), (1,)), ((), ())), preferred_element_type=jnp.float32)
        scores = scores + bias_ref[head] + mask
        top = jnp.max(scores, axis=-1, keepdims=True)
        weights = jnp.exp(scores - top)
        total = jnp.sum(weights, axis=-1, keepdims=True)
        probs = (weights * (1.0 / total)).astype(jnp.bfloat16)
        out = jnp.dot(probs, v_ref[:, cols], preferred_element_type=jnp.float32)
        o_ref[:, cols] = out.astype(jnp.bfloat16)


def attention_core(query, key, value, rel_bias, mask_add, num_seqs):
    num_heads, seq_len, _ = rel_bias.shape
    head_dim = query.shape[1] // num_heads
    step = HEADS_PER_STEP
    rows = pl.BlockSpec((seq_len, step * head_dim), lambda h, s: (s, h))
    return pl.pallas_call(
        functools.partial(attn_kernel, head_dim),
        grid=(num_heads // step, num_seqs),
        in_specs=[rows, rows, rows, pl.BlockSpec((step, seq_len, seq_len), lambda h, s: (h, 0, 0)), pl.BlockSpec((1, 1, seq_len), lambda h, s: (s, 0, 0))],
        out_specs=rows,
        out_shape=jax.ShapeDtypeStruct(query.shape, jnp.bfloat16),
        compiler_params=pltpu.CompilerParams(vmem_limit_bytes=48 * 1024 * 1024),
        cost_estimate=pl.CostEstimate(flops=4 * num_seqs * seq_len * seq_len * query.shape[1], bytes_accessed=8 * query.size + 4 * rel_bias.size, transcendentals=num_seqs * num_heads * seq_len * seq_len),
        name="attn_core",
    )(query, key, value, rel_bias, mask_add)


def attention(flat, mask_add, rel_bias, gain, query_w, key_w, value_w, out_w, num_seqs):
    normed = rms_norm(flat, gain).astype(jnp.bfloat16)

    def project(weight):
        return jnp.dot(normed, weight, preferred_element_type=jnp.float32).astype(jnp.bfloat16)

    context = attention_core(project(query_w), project(key_w), project(value_w), rel_bias, mask_add, num_seqs)
    attn_out = jnp.dot(context, out_w, preferred_element_type=jnp.float32)
    return (flat.astype(jnp.float32) + attn_out).astype(jnp.bfloat16)


def route_tables(expert_ids, num_experts, capacity):
    tok_count = expert_ids.shape[1]
    member = expert_ids[:, :, None] == jnp.arange(num_experts, dtype=jnp.int32)
    tok = jnp.arange(tok_count, dtype=jnp.int32)
    earlier = (tok[:, None] > tok[None, :]).astype(jnp.bfloat16)
    ranks = jnp.einsum('ts,lse->lte', earlier, member.astype(jnp.bfloat16), preferred_element_type=jnp.float32)
    slot = jnp.sum(jnp.where(member, ranks, 0.0), axis=-1).astype(jnp.int32)
    in_slot = (slot[:, :, None] == jnp.arange(capacity, dtype=jnp.int32)).astype(jnp.bfloat16)
    high = (tok // 32).astype(jnp.bfloat16)[None, :, None] * in_slot
    low = (tok % 32).astype(jnp.bfloat16)[None, :, None] * in_slot
    parts = jnp.einsum('lte,ltc->lec', member.astype(jnp.bfloat16), jnp.concatenate([high, low], axis=-1), preferred_element_type=jnp.float32)
    parts = parts.astype(jnp.int32)
    slot_token = parts[:, :, :capacity] * 32 + parts[:, :, capacity:]
    return member, slot, slot_token


def gate_values(normed32, route_w, member):
    logits = jnp.dot(normed32, route_w, precision=lax.Precision.HIGHEST, preferred_element_type=jnp.float32)
    return jnp.sum(jnp.where(member, jax.nn.softmax(logits, axis=-1), 0.0), axis=-1)


def solution(mesh):
    token_spec = P(('dp', 'ep'))
    groups = mesh.shape['ep']

    def per_device(x_in, pad_mask, rel_bias, expert_idx, norm_scale, w_query, w_key, w_value, w_attn_out, w_router, w_in, w_out):
        num_seqs, seq_len, model_dim = x_in.shape
        tok_count = num_seqs * seq_len
        num_layers, _, num_experts = w_router.shape
        capacity = (CAP_FACTOR * tok_count + num_experts - 1) // num_experts
        local = num_experts // groups
        flat_ids = expert_idx.reshape(num_layers, tok_count)
        member, slot, slot_token = route_tables(flat_ids, num_experts, capacity)
        kept = slot < capacity
        back = (flat_ids // local) * capacity + jnp.minimum(slot, capacity - 1)
        which = flat_ids % local
        mask_add = jnp.where(pad_mask > 0, 0.0, NEG_BIG).astype(jnp.float32)[:, None, :]
        flat = x_in.reshape(tok_count, model_dim)
        for lay in range(num_layers):
            flat = attention(flat, mask_add, rel_bias, norm_scale[lay, 0], w_query[lay], w_key[lay], w_value[lay], w_attn_out[lay], num_seqs)
            normed32 = rms_norm(flat, norm_scale[lay, 1])
            rows = normed32.astype(jnp.bfloat16)
            sources = slot_token[lay].reshape(groups, local, capacity)
            for loc in range(local):
                packed = jnp.take(rows, sources[:, loc].reshape(-1), axis=0, mode='clip')
                received = lax.all_to_all(packed, 'ep', 0, 0, tiled=True)
                inner = jnp.dot(received, w_in[lay, loc], preferred_element_type=jnp.float32)
                inner = jnp.maximum(inner, 0.0).astype(jnp.bfloat16)
                outer = jnp.dot(inner, w_out[lay, loc], preferred_element_type=jnp.float32).astype(jnp.bfloat16)
                returned = lax.all_to_all(outer, 'ep', 0, 0, tiled=True)
                mine = jnp.take(returned, back[lay], axis=0, mode='clip')
                update = jnp.where((which[lay] == loc)[:, None], mine, update) if loc else mine
            gate = gate_values(normed32, w_router[lay], member[lay])
            scale = jnp.where(kept[lay], gate, 0.0)[:, None]
            flat = (flat.astype(jnp.float32) + scale * update.astype(jnp.float32)).astype(jnp.bfloat16)
        return flat.reshape(num_seqs, seq_len, model_dim)

    return jax.shard_map(per_device, mesh=mesh, in_specs=(token_spec, token_spec, P(), P(None, ('dp', 'ep')), P(), P(), P(), P(), P(), P(), P(None, 'ep'), P(None, 'ep')), out_specs=token_spec, check_vma=False)
```

```python
import functools

import jax
import jax.numpy as jnp
from jax import lax
from jax.experimental import pallas as pl
from jax.experimental.pallas import tpu as pltpu
from jax.sharding import PartitionSpec as P

NORM_EPS = 1e-6
NEG_BIG = -1e9
CAP_FACTOR = 2
HEADS_PER_STEP = 4


def rms_norm(hidden, gain):
    hid32 = hidden.astype(jnp.float32)
    return hid32 * lax.rsqrt(jnp.mean(hid32 * hid32, axis=-1, keepdims=True) + NORM_EPS) * gain


def attn_kernel(head_dim, q_ref, k_ref, v_ref, bias_ref, mask_ref, o_ref):
    mask = mask_ref[0]
    heads = bias_ref.shape[0]

    def score(head):
        cols = slice(head * head_dim, (head + 1) * head_dim)
        return lax.dot_general(q_ref[:, cols], k_ref[:, cols], (((1,), (1,)), ((), ())), preferred_element_type=jnp.float32)

    ahead = score(0)
    prev = None
    for head in range(heads + 1):
        if head < heads:
            scores = ahead + bias_ref[head] + mask
            if head + 1 < heads:
                ahead = score(head + 1)
            top = jnp.max(scores, axis=-1, keepdims=True)
            weights = jnp.exp(scores - top)
            total = jnp.sum(weights, axis=-1, keepdims=True)
            probs = (weights * (1.0 / total)).astype(jnp.bfloat16)
        if prev is not None:
            cols = slice((head - 1) * head_dim, head * head_dim)
            o_ref[:, cols] = jnp.dot(prev, v_ref[:, cols], preferred_element_type=jnp.float32).astype(jnp.bfloat16)
        prev = probs


def attention_core(query, key, value, rel_bias, mask_add, num_seqs):
    num_heads, seq_len, _ = rel_bias.shape
    head_dim = query.shape[1] // num_heads
    step = HEADS_PER_STEP
    rows = pl.BlockSpec((seq_len, step * head_dim), lambda h, s: (s, h))
    return pl.pallas_call(
        functools.partial(attn_kernel, head_dim),
        grid=(num_heads // step, num_seqs),
        in_specs=[rows, rows, rows, pl.BlockSpec((step, seq_len, seq_len), lambda h, s: (h, 0, 0)), pl.BlockSpec((1, 1, seq_len), lambda h, s: (s, 0, 0))],
        out_specs=rows,
        out_shape=jax.ShapeDtypeStruct(query.shape, jnp.bfloat16),
        compiler_params=pltpu.CompilerParams(vmem_limit_bytes=48 * 1024 * 1024),
        cost_estimate=pl.CostEstimate(flops=4 * num_seqs * seq_len * seq_len * query.shape[1], bytes_accessed=8 * query.size + 4 * rel_bias.size, transcendentals=num_seqs * num_heads * seq_len * seq_len),
        name="attn_core",
    )(query, key, value, rel_bias, mask_add)


def attention(flat, mask_add, rel_bias, gain, query_w, key_w, value_w, out_w, num_seqs):
    normed = rms_norm(flat, gain).astype(jnp.bfloat16)

    def project(weight):
        return jnp.dot(normed, weight, preferred_element_type=jnp.float32).astype(jnp.bfloat16)

    context = attention_core(project(query_w), project(key_w), project(value_w), rel_bias, mask_add, num_seqs)
    attn_out = jnp.dot(context, out_w, preferred_element_type=jnp.float32)
    return (flat.astype(jnp.float32) + attn_out).astype(jnp.bfloat16)


def route_tables(expert_ids, num_experts, capacity):
    tok_count = expert_ids.shape[1]
    member = expert_ids[:, :, None] == jnp.arange(num_experts, dtype=jnp.int32)
    tok = jnp.arange(tok_count, dtype=jnp.int32)
    earlier = (tok[:, None] > tok[None, :]).astype(jnp.bfloat16)
    ranks = jnp.einsum('ts,lse->lte', earlier, member.astype(jnp.bfloat16), preferred_element_type=jnp.float32)
    slot = jnp.sum(jnp.where(member, ranks, 0.0), axis=-1).astype(jnp.int32)
    return member, slot


def gate_values(normed32, route_w, member):
    logits = jnp.dot(normed32, route_w, precision=lax.Precision.HIGHEST, preferred_element_type=jnp.float32)
    return jnp.sum(jnp.where(member, jax.nn.softmax(logits, axis=-1), 0.0), axis=-1)


def solution(mesh):
    token_spec = P(('dp', 'ep'))
    groups = mesh.shape['ep']

    def per_device(x_in, pad_mask, rel_bias, expert_idx, norm_scale, w_query, w_key, w_value, w_attn_out, w_router, w_in, w_out):
        num_seqs, seq_len, model_dim = x_in.shape
        tok_count = num_seqs * seq_len
        num_layers, _, num_experts = w_router.shape
        capacity = (CAP_FACTOR * tok_count + num_experts - 1) // num_experts
        local = num_experts // groups
        flat_ids = expert_idx.reshape(num_layers, tok_count)
        member, slot = route_tables(flat_ids, num_experts, capacity)
        row = jnp.where(slot < capacity, (flat_ids // local) * capacity + slot, -1)
        which = flat_ids % local
        row_ids = jnp.arange(groups * capacity, dtype=jnp.int32)
        mask_add = jnp.where(pad_mask > 0, 0.0, NEG_BIG).astype(jnp.float32)[:, None, :]
        flat = x_in.reshape(tok_count, model_dim)
        for lay in range(num_layers):
            flat = attention(flat, mask_add, rel_bias, norm_scale[lay, 0], w_query[lay], w_key[lay], w_value[lay], w_attn_out[lay], num_seqs)
            normed32 = rms_norm(flat, norm_scale[lay, 1])
            rows = normed32.astype(jnp.bfloat16)
            update = None
            for loc in range(local):
                place = jnp.where(which[lay] == loc, row[lay], -1)
                moves = (row_ids[:, None] == place[None, :]).astype(jnp.bfloat16)
                packed = jnp.dot(moves, rows, preferred_element_type=jnp.float32).astype(jnp.bfloat16)
                received = lax.all_to_all(packed, 'ep', 0, 0, tiled=True)
                inner = jnp.dot(received, w_in[lay, loc], preferred_element_type=jnp.float32)
                inner = jnp.maximum(inner, 0.0).astype(jnp.bfloat16)
                outer = jnp.dot(inner, w_out[lay, loc], preferred_element_type=jnp.float32).astype(jnp.bfloat16)
                returned = lax.all_to_all(outer, 'ep', 0, 0, tiled=True)
                mine = lax.dot_general(moves, returned, (((0,), (0,)), ((), ())), preferred_element_type=jnp.float32)
                update = mine if update is None else update.astype(jnp.float32) + mine
                if loc < local - 1:
                    update = update.astype(jnp.bfloat16)
            gate = gate_values(normed32, w_router[lay], member[lay])
            flat = (flat.astype(jnp.float32) + gate[:, None] * update).astype(jnp.bfloat16)
        return flat.reshape(num_seqs, seq_len, model_dim)

    return jax.shard_map(per_device, mesh=mesh, in_specs=(token_spec, token_spec, P(), P(None, ('dp', 'ep')), P(), P(), P(), P(), P(), P(), P(None, 'ep'), P(None, 'ep')), out_specs=token_spec, check_vma=False)
```

```python
import functools

import jax
import jax.numpy as jnp
from jax import lax
from jax.experimental import pallas as pl
from jax.experimental.pallas import tpu as pltpu
from jax.sharding import PartitionSpec as P

NORM_EPS = 1e-6
NEG_BIG = -1e9
CAP_FACTOR = 2
HEADS_PER_STEP = 4


def rms_norm(hidden, gain):
    hid32 = hidden.astype(jnp.float32)
    return hid32 * lax.rsqrt(jnp.mean(hid32 * hid32, axis=-1, keepdims=True) + NORM_EPS) * gain


def attn_kernel(head_dim, q_ref, k_ref, v_ref, bias_ref, mask_ref, o_ref):
    mask = mask_ref[0]
    heads = bias_ref.shape[0]

    def score(head):
        cols = slice(head * head_dim, (head + 1) * head_dim)
        return lax.dot_general(q_ref[:, cols], k_ref[:, cols], (((1,), (1,)), ((), ())), preferred_element_type=jnp.float32)

    ahead = score(0)
    prev = None
    for head in range(heads + 1):
        if head < heads:
            scores = ahead + bias_ref[head] + mask
            if head + 1 < heads:
                ahead = score(head + 1)
            top = jnp.max(scores, axis=-1, keepdims=True)
            weights = jnp.exp(scores - top)
            total = jnp.sum(weights, axis=-1, keepdims=True)
            probs = (weights * (1.0 / total)).astype(jnp.bfloat16)
        if prev is not None:
            cols = slice((head - 1) * head_dim, head * head_dim)
            o_ref[:, cols] = jnp.dot(prev, v_ref[:, cols], preferred_element_type=jnp.float32).astype(jnp.bfloat16)
        prev = probs


def attention_core(query, key, value, rel_bias, mask_add, num_seqs):
    num_heads, seq_len, _ = rel_bias.shape
    head_dim = query.shape[1] // num_heads
    step = HEADS_PER_STEP
    rows = pl.BlockSpec((seq_len, step * head_dim), lambda h, s: (s, h))
    return pl.pallas_call(
        functools.partial(attn_kernel, head_dim),
        grid=(num_heads // step, num_seqs),
        in_specs=[rows, rows, rows, pl.BlockSpec((step, seq_len, seq_len), lambda h, s: (h, 0, 0)), pl.BlockSpec((1, 1, seq_len), lambda h, s: (s, 0, 0))],
        out_specs=rows,
        out_shape=jax.ShapeDtypeStruct(query.shape, jnp.bfloat16),
        compiler_params=pltpu.CompilerParams(vmem_limit_bytes=48 * 1024 * 1024),
        cost_estimate=pl.CostEstimate(flops=4 * num_seqs * seq_len * seq_len * query.shape[1], bytes_accessed=8 * query.size + 4 * rel_bias.size, transcendentals=num_seqs * num_heads * seq_len * seq_len),
        name="attn_core",
    )(query, key, value, rel_bias, mask_add)


def project_kernel(hid_ref, gain_ref, query_w, key_w, value_w, query_ref, key_ref, value_ref, normed_ref):
    tile = 128

    @pl.when(pl.program_id(0) == 0)
    def _():
        @pl.loop(0, hid_ref.shape[0] // tile)
        def _(step):
            rows = pl.ds(pl.multiple_of(step * tile, tile), tile)
            normed_ref[rows, :] = rms_norm(hid_ref[rows, :], gain_ref[...]).astype(jnp.bfloat16)

    for weight, out in ((query_w, query_ref), (key_w, key_ref), (value_w, value_ref)):
        out[...] = jnp.dot(normed_ref[...], weight[0], preferred_element_type=jnp.float32).astype(jnp.bfloat16)


def project(layer, flat, gain, query_w, key_w, value_w):
    tok_count, model_dim = flat.shape
    inner = query_w.shape[2]
    cols = 512
    weight = pl.BlockSpec((1, model_dim, cols), lambda n: (layer, 0, n))
    out = pl.BlockSpec((tok_count, cols), lambda n: (0, n))
    return pl.pallas_call(
        project_kernel,
        grid=(inner // cols,),
        in_specs=[pl.BlockSpec((tok_count, model_dim), lambda n: (0, 0), pipeline_mode=pl.Buffered(1)), pl.BlockSpec((1, model_dim), lambda n: (0, 0)), weight, weight, weight],
        out_specs=(out, out, out),
        out_shape=(jax.ShapeDtypeStruct((tok_count, inner), jnp.bfloat16),) * 3,
        scratch_shapes=[pltpu.VMEM((tok_count, model_dim), jnp.bfloat16)],
        compiler_params=pltpu.CompilerParams(vmem_limit_bytes=56 * 1024 * 1024),
        cost_estimate=pl.CostEstimate(flops=6 * tok_count * model_dim * inner, bytes_accessed=8 * flat.size + 6 * model_dim * inner, transcendentals=0),
        name="project",
    )(flat, gain[None, :], query_w, key_w, value_w)


def attention(layer, flat, mask_add, rel_bias, gain, query_w, key_w, value_w, out_w, num_seqs):
    query, key, value = project(layer, flat, gain, query_w, key_w, value_w)
    context = attention_core(query, key, value, rel_bias, mask_add, num_seqs)
    attn_out = jnp.dot(context, out_w, preferred_element_type=jnp.float32)
    return (flat.astype(jnp.float32) + attn_out).astype(jnp.bfloat16)


def route_tables(expert_ids, num_experts, capacity):
    tok_count = expert_ids.shape[1]
    member = expert_ids[:, :, None] == jnp.arange(num_experts, dtype=jnp.int32)
    tok = jnp.arange(tok_count, dtype=jnp.int32)
    earlier = (tok[:, None] > tok[None, :]).astype(jnp.bfloat16)
    ranks = jnp.einsum('ts,lse->lte', earlier, member.astype(jnp.bfloat16), preferred_element_type=jnp.float32)
    slot = jnp.sum(jnp.where(member, ranks, 0.0), axis=-1).astype(jnp.int32)
    return member, slot


def gate_values(normed32, route_w, member):
    logits = jnp.dot(normed32, route_w, precision=lax.Precision.HIGHEST, preferred_element_type=jnp.float32)
    return jnp.sum(jnp.where(member, jax.nn.softmax(logits, axis=-1), 0.0), axis=-1)


def solution(mesh):
    token_spec = P(('dp', 'ep'))
    groups = mesh.shape['ep']

    def per_device(x_in, pad_mask, rel_bias, expert_idx, norm_scale, w_query, w_key, w_value, w_attn_out, w_router, w_in, w_out):
        num_seqs, seq_len, model_dim = x_in.shape
        tok_count = num_seqs * seq_len
        num_layers, _, num_experts = w_router.shape
        capacity = (CAP_FACTOR * tok_count + num_experts - 1) // num_experts
        local = num_experts // groups
        flat_ids = expert_idx.reshape(num_layers, tok_count)
        member, slot = route_tables(flat_ids, num_experts, capacity)
        row = jnp.where(slot < capacity, (flat_ids // local) * capacity + slot, -1)
        which = flat_ids % local
        row_ids = jnp.arange(groups * capacity, dtype=jnp.int32)
        mask_add = jnp.where(pad_mask > 0, 0.0, NEG_BIG).astype(jnp.float32)[:, None, :]
        flat = x_in.reshape(tok_count, model_dim)
        for lay in range(num_layers):
            flat = attention(lay, flat, mask_add, rel_bias, norm_scale[lay, 0], w_query, w_key, w_value, w_attn_out[lay], num_seqs)
            normed32 = rms_norm(flat, norm_scale[lay, 1])
            rows = normed32.astype(jnp.bfloat16)
            update = None
            for loc in range(local):
                place = jnp.where(which[lay] == loc, row[lay], -1)
                moves = (row_ids[:, None] == place[None, :]).astype(jnp.bfloat16)
                packed = jnp.dot(moves, rows, preferred_element_type=jnp.float32).astype(jnp.bfloat16)
                received = lax.all_to_all(packed, 'ep', 0, 0, tiled=True)
                inner = jnp.dot(received, w_in[lay, loc], preferred_element_type=jnp.float32)
                inner = jnp.maximum(inner, 0.0).astype(jnp.bfloat16)
                outer = jnp.dot(inner, w_out[lay, loc], preferred_element_type=jnp.float32).astype(jnp.bfloat16)
                returned = lax.all_to_all(outer, 'ep', 0, 0, tiled=True)
                mine = lax.dot_general(moves, returned, (((0,), (0,)), ((), ())), preferred_element_type=jnp.float32)
                update = mine if update is None else update.astype(jnp.float32) + mine
                if loc < local - 1:
                    update = update.astype(jnp.bfloat16)
            gate = gate_values(normed32, w_router[lay], member[lay])
            flat = (flat.astype(jnp.float32) + gate[:, None] * update).astype(jnp.bfloat16)
        return flat.reshape(num_seqs, seq_len, model_dim)

    return jax.shard_map(per_device, mesh=mesh, in_specs=(token_spec, token_spec, P(), P(None, ('dp', 'ep')), P(), P(), P(), P(), P(), P(), P(None, 'ep'), P(None, 'ep')), out_specs=token_spec, check_vma=False)
```
